32 devices in a mesh: groups: 2 (over x), ep: 16 (over z, y, core).
Axes of the slice: x: 2, y: 2, z: 4, core: 2. Of those that a mesh axis runs over, the one named last changes fastest.
Arguments:
- tokens: bfloat16 [256, 7168], P(('groups', 'ep')), parts along dimension 0, may hold values from -6 to 6
- experts: int32 [256, 8], P(('groups', 'ep')), parts along dimension 0, may hold values from 0 to 15, as said below
- gate_fixed: int32 [256, 8], P(('groups', 'ep')), parts along dimension 0, may hold values from 1 to 65535
- home_slot: int32 [256], P(('groups', 'ep')), parts along dimension 0, may hold values from 0 to 7, as said below
- bias: float32 [16], replicated, may hold values from -0.5 to 0.5
- w_gate: bfloat16 [7168, 32768], P(None, 'ep'), may hold values from -0.0625 to 0.0625
- w_up: bfloat16 [7168, 32768], P(None, 'ep'), may hold values from -0.0625 to 0.0625
- w_down: bfloat16 [32768, 7168], P('ep'), may hold values from -0.125 to 0.125
Outputs:
- moe_out: bfloat16 [256, 7168], P(('groups', 'ep')), parts along dimension 0
- bias_next: float32 [32], P('groups'), parts along dimension 0
The draws below stay inside these ranges and needn't reach their ends.
There are 2 independent parts, one for each index of `groups`. The reference program is written for one: setup_inputs(seed, part) draws one part's arguments, and reference() takes and returns one part's arrays. A program takes and returns all parts, laid end to end along the dimension named above; an argument that names none is the same for every part. Nothing has to cross between parts.
Inputs may be any that keep to these rules, and one draw needn't show every extreme that they name: Each token names 8 different experts; among the tokens of one device no expert is named more than 6 times, and some device reaches that bound. `home_slot`: within each device's block of 8 tokens every value appears exactly once.
All inputs are finite; a program needn't handle non-finite values.
Results may differ from the reference program's by a relative error of at most 0.008.
Values may be sent and summed in bfloat16 or wider, within the bound.
No kernel may reach another device: no remote copies, remote signals or barrier semaphores. Data moves between devices by JAX's collectives and lax.ppermute only.
A program may use at most 128 MiB of HBM per device.

```python
import math
import jax
import jax.numpy as jnp
from jax import lax

D = 7168
FF = 2048
TOP = 8
EXPERTS = 16
TOK_DEV = 8
SHARDS = 1
FF_DEV = 2048
TOKENS = 128
CAP = 6
N_EP = 16


def draw_home_slot(key, part):
    block_count = TOKENS // TOK_DEV
    scores = jax.random.randint(key, (block_count, TOK_DEV), 0, 1 << 20, dtype=jnp.int32)
    scores = scores * TOK_DEV + jnp.arange(TOK_DEV, dtype=jnp.int32)[None, :]
    ordering = jnp.argsort(scores, axis=1, stable=True).astype(jnp.int32)
    return ordering.reshape(TOKENS)


def draw_experts(key, part):
    block_count = TOKENS // TOK_DEV
    pair_count = TOK_DEV * TOP
    narrow = min(EXPERTS, max(TOP, -(-pair_count // CAP)))
    base = jax.random.fold_in(key, 17)
    first_key = jax.random.fold_in(base, 1)
    second_key = jax.random.fold_in(base, 2)
    third_key = jax.random.fold_in(base, 3)
    common_scores = jax.random.randint(first_key, (EXPERTS,), 0, 1 << 20, dtype=jnp.int32)
    common_scores = common_scores * EXPERTS + jnp.arange(EXPERTS, dtype=jnp.int32)
    common = jnp.argsort(common_scores, stable=True).astype(jnp.int32)
    block_scores = jax.random.randint(second_key, (block_count, EXPERTS), 0, 1 << 20, dtype=jnp.int32)
    block_scores = block_scores * EXPERTS + jnp.arange(EXPERTS, dtype=jnp.int32)[None, :]
    block_order = jnp.argsort(block_scores, axis=1, stable=True).astype(jnp.int32)
    coin = jax.random.randint(third_key, (block_count,), 0, max(block_count - 1, 1), dtype=jnp.int32)
    concentrated = coin < jnp.arange(block_count, dtype=jnp.int32)
    pair_index = jnp.arange(pair_count, dtype=jnp.int32)
    hot_ids = common[pair_index % narrow]
    spread_index = jnp.broadcast_to((pair_index % EXPERTS)[None, :], (block_count, pair_count))
    spread_ids = jnp.take_along_axis(block_order, spread_index, axis=1)
    chosen = jnp.where(concentrated[:, None], hot_ids[None, :], spread_ids)
    return chosen.reshape(TOKENS, TOP).astype(jnp.int32)


def plant(values, rng, least, high):
    place = [jax.random.randint(jax.random.fold_in(rng, axis), (), 0, length) for axis, length in enumerate(values.shape)]
    longest = values.shape.index(max(values.shape))
    neighbour = place[:longest] + [(place[longest] + 1) % values.shape[longest]] + place[longest + 1:]
    return values.at[tuple(place)].set(least).at[tuple(neighbour)].set(high)


def block_levels(stream_key, shape, cuts, smallest, largest):
    def one(dim, blocks):
        draws = jax.random.uniform(jax.random.fold_in(jax.random.fold_in(stream_key, 6), dim), (blocks,), jnp.float32, smallest / len(cuts), largest / len(cuts))
        return jnp.repeat(jnp.exp(draws), shape[dim] // blocks).reshape((-1,) + (1,) * (len(shape) - dim - 1))

    factor_of = one(*cuts[0])
    for cut in cuts[1:]:
        factor_of = factor_of * one(*cut)
    return factor_of


def normal_values(stream_key, extent, deviation, reach, split=(), kind=jnp.bfloat16):
    factor_of = block_levels(stream_key, extent, split, -0.22, 0.18) if split else 1.0
    result = jax.random.normal(stream_key, extent, jnp.float32) * deviation * factor_of
    return jnp.minimum(jnp.maximum(result, -reach), reach).astype(kind)


def setup_inputs(seed: int = 0, part: int = 0) -> dict:
    key_list = jax.random.split(jax.random.key(seed), 9)
    part_keys = jax.random.split(jax.random.fold_in(key_list[8], part), 9)
    tokens = normal_values(part_keys[0], (TOKENS, D), 1.0, 6.0, ((0, 16),))
    experts = draw_experts(jax.random.fold_in(jax.random.fold_in(key_list[8], part), 71), part)
    gate_fixed = plant(jax.random.randint(part_keys[2], (TOKENS, TOP), 1, 65536), jax.random.fold_in(part_keys[2], 1), 1, 65535).astype(jnp.int32)
    home_slot = draw_home_slot(jax.random.fold_in(jax.random.fold_in(key_list[8], part), 71), part)
    bias = jnp.clip(jax.random.uniform(key_list[4], (EXPERTS,), jnp.float32, -0.5, 0.5), -0.5, 0.5)
    w_gate = normal_values(key_list[5], (D, EXPERTS * FF), D ** -0.5, 0.0625, ((1, 16),))
    w_up = normal_values(key_list[6], (D, EXPERTS * FF), D ** -0.5, 0.0625, ((1, 16),))
    w_down = normal_values(key_list[7], (EXPERTS * FF, D), FF ** -0.5, 0.125, ((0, 16),))
    return dict(tokens=tokens, experts=experts, gate_fixed=gate_fixed, home_slot=home_slot, bias=bias, w_gate=w_gate, w_up=w_up, w_down=w_down)


ROUTED_SCALE = 2.5

def reference(tokens, experts, gate_fixed, home_slot, bias, w_gate, w_up, w_down):
    pair_count = TOK_DEV * TOP
    flat_ids = experts.reshape(N_EP, pair_count)
    hit_table = (flat_ids[:, :, None] == jnp.arange(EXPERTS, dtype=jnp.int32)[None, None, :]).astype(jnp.int32)
    earlier = jnp.cumsum(hit_table, axis=1) - hit_table
    slot_rank = lax.optimization_barrier(jnp.sum(earlier * hit_table, axis=2)).astype(jnp.int32)
    pair_token = jnp.arange(N_EP, dtype=jnp.int32)[:, None] * TOK_DEV + jnp.arange(pair_count, dtype=jnp.int32)[None, :] // TOP
    position = ((jnp.arange(N_EP, dtype=jnp.int32)[:, None] * EXPERTS + flat_ids) * CAP + slot_rank).reshape(-1)
    fixed_gate = gate_fixed.astype(jnp.float32)
    gate_share = ROUTED_SCALE * fixed_gate / lax.optimization_barrier(jnp.sum(fixed_gate, axis=1, keepdims=True))
    source_table = jnp.full((N_EP * EXPERTS * CAP,), -1, jnp.int32).at[position].set(pair_token.reshape(-1))
    source_table = source_table.reshape(N_EP, EXPERTS, CAP)
    share_table = jnp.zeros((N_EP * EXPERTS * CAP,), jnp.float32).at[position].set(gate_share.reshape(-1))
    share_table = share_table.reshape(N_EP, EXPERTS, CAP)

    def one_expert(running, expert_id):
        index_rows = lax.dynamic_index_in_dim(source_table, expert_id, 1, keepdims=False).reshape(-1)
        share_rows = lax.dynamic_index_in_dim(share_table, expert_id, 1, keepdims=False).reshape(-1)
        valid = index_rows >= 0
        safe_rows = jnp.maximum(index_rows, 0)
        row_block = jnp.where(valid[:, None], tokens[safe_rows], jnp.zeros((), jnp.bfloat16))
        first = (expert_id * FF).astype(jnp.int32)
        gate_cols = lax.dynamic_slice_in_dim(w_gate, first, FF, 1)
        up_cols = lax.dynamic_slice_in_dim(w_up, first, FF, 1)
        down_rows = lax.dynamic_slice_in_dim(w_down, first, FF, 0)
        gate_part = jnp.dot(row_block, gate_cols, preferred_element_type=jnp.float32)
        up_part = jnp.dot(row_block, up_cols, preferred_element_type=jnp.float32)
        hidden = (jax.nn.silu(gate_part) * up_part).astype(jnp.bfloat16)
        row_count = hidden.shape[0]
        hidden_groups = hidden.astype(jnp.float32).reshape(row_count, SHARDS, FF_DEV)
        down_groups = down_rows.astype(jnp.float32).reshape(SHARDS, FF_DEV, D)
        partial_value = jnp.einsum('rsf,sfd->rsd', hidden_groups, down_groups).astype(jnp.bfloat16)
        expert_out = lax.optimization_barrier(jnp.sum(partial_value.astype(jnp.float32), axis=1))
        weighted = jnp.where(valid[:, None], expert_out * share_rows[:, None], jnp.zeros((), jnp.float32))
        return (running.at[safe_rows].add(weighted), None)
    start = jnp.zeros((N_EP * TOK_DEV, D), jnp.float32)
    summed, _ = lax.scan(one_expert, start, jnp.arange(EXPERTS, dtype=jnp.int32))
    combined = summed.astype(jnp.bfloat16).reshape(N_EP, TOK_DEV, D)
    block_ids = jnp.broadcast_to(jnp.arange(N_EP, dtype=jnp.int32)[:, None], (N_EP, TOK_DEV))
    placed = jnp.zeros((N_EP, TOK_DEV, D), jnp.bfloat16).at[block_ids, home_slot.reshape(N_EP, TOK_DEV)].set(combined)
    moe_out = placed.reshape(N_EP * TOK_DEV, D)
    load = lax.optimization_barrier(jnp.sum(hit_table, axis=(0, 1))).astype(jnp.float32)
    average = N_EP * TOK_DEV * TOP / EXPERTS
    bias_next = bias + 2.0 / math.sqrt(average) * (average - load)
    return (moe_out, bias_next)
```

```python
import math

import jax
import jax.numpy as jnp
from jax import lax
from jax.experimental import pallas as pl
from jax.experimental.pallas import tpu as pltpu
from jax.sharding import PartitionSpec as P

ROUTED_SCALE = 2.5
LANES = 128
VMEM = pl.BlockSpec(memory_space=pltpu.VMEM)
ANY = pl.BlockSpec(memory_space=pl.ANY)
SMEM = pl.BlockSpec(memory_space=pltpu.SMEM)
MIB = 1 << 20


def divisor(total, want, step):
    best = step
    for size in range(step, min(total, want) + 1, step):
        if total % size == 0:
            best = size
    return best


def pack_rows(tokens, experts, gate_fixed, home_slot, expert_count):
    rows, width = tokens.shape
    top = experts.shape[1]
    extra = -(-2 * expert_count // LANES) * LANES

    def kernel(tok_ref, exp_ref, gate_ref, home_ref, out_ref):
        row = lax.broadcasted_iota(jnp.int32, (rows, rows), 0)
        col = lax.broadcasted_iota(jnp.int32, (rows, rows), 1)
        placer = jnp.zeros((rows, rows), jnp.float32)
        for t in range(rows):
            placer = jnp.where((col == t) & (row == home_ref[t]), 1.0, placer)
        placer = placer.astype(jnp.bfloat16)
        out_ref[:, :width] = jnp.dot(
            placer, tok_ref[...], preferred_element_type=jnp.float32
        ).astype(jnp.bfloat16)
        lane = lax.broadcasted_iota(jnp.int32, (rows, extra), 1)
        below = gate_ref[...] - 1
        low, high = (below & 255) + 1, below >> 8
        meta = jnp.zeros((rows, extra), jnp.int32)
        for k in range(top):
            chosen = exp_ref[:, k : k + 1]
            meta = jnp.where(lane == chosen, low[:, k : k + 1], meta)
            meta = jnp.where(lane == chosen + expert_count, high[:, k : k + 1], meta)
        out_ref[:, width:] = jnp.dot(
            placer, meta.astype(jnp.float32).astype(jnp.bfloat16), preferred_element_type=jnp.float32
        ).astype(jnp.bfloat16)

    return pl.pallas_call(
        kernel,
        out_shape=jax.ShapeDtypeStruct((rows, width + extra), jnp.bfloat16),
        in_specs=[VMEM, VMEM, VMEM, SMEM],
        out_specs=VMEM,
        compiler_params=pltpu.CompilerParams(vmem_limit_bytes=4 * MIB),
        name="pack_rows",
    )(tokens, experts, gate_fixed, home_slot)


def expert_partials(blocks, w_gate, w_up, w_down, expert_count, shards, pieces):
    count = len(blocks)
    rows = blocks[0].shape[0]
    width, units = w_gate.shape
    extra = blocks[0].shape[1] - width
    total = count * rows
    half = total // 2
    up_cols = divisor(units, 256, LANES)
    piece = width // pieces
    down_cols = divisor(piece, 1024, LANES)
    up_steps, down_steps, per_piece = units // up_cols, width // down_cols, piece // down_cols
    slots, down_slots = min(3, up_steps), min(3, down_steps)

    def kernel(*refs):
        block_refs = refs[:count]
        gate_hbm, up_hbm, down_hbm = refs[count : count + 3]
        outs = refs[count + 3 : count + 3 + 2 * pieces]
        load_ref = refs[count + 3 + 2 * pieces]
        x, meta, hidden, gate_buf, up_buf, down_buf, gate_sem, up_sem, down_sem = refs[count + 4 + 2 * pieces :]

        def gate_copy(n):
            cols = pl.ds(pl.multiple_of(n * up_cols, up_cols), up_cols)
            return pltpu.make_async_copy(gate_hbm.at[:, cols], gate_buf.at[n % slots], gate_sem.at[n % slots])

        def up_copy(n):
            cols = pl.ds(pl.multiple_of(n * up_cols, up_cols), up_cols)
            return pltpu.make_async_copy(up_hbm.at[:, cols], up_buf.at[n % slots], up_sem.at[n % slots])

        def down_copy(n):
            cols = pl.ds(pl.multiple_of(n * down_cols, LANES), down_cols)
            return pltpu.make_async_copy(down_hbm.at[:, cols], down_buf.at[n % down_slots], down_sem.at[n % down_slots])

        for n in range(slots):
            gate_copy(n).start()
            up_copy(n).start()
        for b in range(count):
            x[b * rows : (b + 1) * rows, :] = block_refs[b][:, :width]
            meta[b * rows : (b + 1) * rows, :] = block_refs[b][:, width:].astype(jnp.float32)
        values = meta[...]
        lane = lax.broadcasted_iota(jnp.int32, (total, extra), 1)
        expert = lax.axis_index("ep") // shards
        is_low, is_high = lane < expert_count, (lane >= expert_count) & (lane < 2 * expert_count)
        scaled = jnp.where(is_high, 256.0 * values, jnp.where(is_low, values, 0.0))
        mine = (lane == expert) | (lane == expert + expert_count)
        own = jnp.sum(jnp.where(mine, scaled, 0.0), axis=1, keepdims=True)
        share = ROUTED_SCALE * own / jnp.sum(scaled, axis=1, keepdims=True)
        load_ref[...] = jnp.sum(jnp.where(is_low & (values > 0.0), 1.0, 0.0), axis=0, keepdims=True)

        def up_step(n, carry):
            @pl.when(n < down_slots)
            def _():
                down_copy(n).start()

            gate_copy(n).wait()
            up_copy(n).wait()
            gate = jnp.dot(x[...], gate_buf[n % slots], preferred_element_type=jnp.float32)
            up = jnp.dot(x[...], up_buf[n % slots], preferred_element_type=jnp.float32)
            cols = pl.ds(pl.multiple_of(n * up_cols, up_cols), up_cols)
            hidden[:, cols] = (gate / (1.0 + jnp.exp(-gate)) * up).astype(jnp.bfloat16)

            @pl.when(n + slots < up_steps)
            def _():
                gate_copy(n + slots).start()
                up_copy(n + slots).start()

            return carry

        lax.fori_loop(0, up_steps, up_step, 0)
        for n in range(min(up_steps, down_slots), down_slots):
            down_copy(n).start()
        for p in range(pieces):

            def down_step(i, carry, p=p):
                n = p * per_piece + i
                down_copy(n).wait()
                out = jnp.dot(hidden[...], down_buf[n % down_slots], preferred_element_type=jnp.float32)
                out = (out * share).astype(jnp.bfloat16)
                cols = pl.ds(pl.multiple_of(i * down_cols, LANES), down_cols)
                outs[2 * p][:, cols] = out[:half]
                outs[2 * p + 1][:, cols] = out[half:]

                @pl.when(n + down_slots < down_steps)
                def _():
                    down_copy(n + down_slots).start()

                return carry

            lax.fori_loop(0, per_piece, down_step, 0)

    shapes = [jax.ShapeDtypeStruct((half, piece), jnp.bfloat16)] * (2 * pieces)
    shapes.append(jax.ShapeDtypeStruct((1, extra), jnp.float32))
    return pl.pallas_call(
        kernel,
        out_shape=shapes,
        in_specs=[VMEM] * count + [ANY] * 3,
        out_specs=[VMEM] * len(shapes),
        scratch_shapes=[
            pltpu.VMEM((total, width), jnp.bfloat16),
            pltpu.VMEM((total, extra), jnp.float32),
            pltpu.VMEM((total, units), jnp.bfloat16),
            pltpu.VMEM((slots, width, up_cols), jnp.bfloat16),
            pltpu.VMEM((slots, width, up_cols), jnp.bfloat16),
            pltpu.VMEM((down_slots, units, down_cols), jnp.bfloat16),
            pltpu.SemaphoreType.DMA((slots,)),
            pltpu.SemaphoreType.DMA((slots,)),
            pltpu.SemaphoreType.DMA((down_slots,)),
        ],
        compiler_params=pltpu.CompilerParams(vmem_limit_bytes=44 * MIB),
        cost_estimate=pl.CostEstimate(
            flops=6 * total * width * units,
            bytes_accessed=6 * width * units,
            transcendentals=total * units,
        ),
        name="expert_partials",
    )(*blocks, w_gate, w_up, w_down)


def per_device(tokens, experts, gate_fixed, home_slot, bias, w_gate, w_up, w_down):
    rows, width = tokens.shape
    top = experts.shape[1]
    expert_count = bias.shape[0]
    devices = lax.axis_size("ep")
    shards = devices // expert_count
    far = devices // 4
    pieces = 2

    def swap(value, mask):
        return lax.ppermute(value, "ep", [(i, i ^ mask) for i in range(devices)])

    own = pack_rows(tokens, experts, gate_fixed, home_slot, expert_count)
    by_z = [own] + [swap(own, 4 * z) for z in range(1, far)]
    by_yz = by_z + [swap(block, 2) for block in by_z]
    blocks = by_yz + [swap(block, 1) for block in by_yz]

    *parts, counts = expert_partials(blocks, w_gate, w_up, w_down, expert_count, shards, pieces)

    f32 = jnp.float32
    quarter = far * rows
    done = []
    for p in range(pieces):
        keep, send = parts[2 * p], parts[2 * p + 1]
        core = swap(send, 1)
        over = (keep[quarter:].astype(f32) + core[quarter:].astype(f32)).astype(jnp.bfloat16)
        side = swap(over, 2)
        summed = keep[:quarter].astype(f32) + core[:quarter].astype(f32) + side.astype(f32)
        total = summed[:rows]
        for z in range(1, far):
            total = total + swap(summed[z * rows : (z + 1) * rows].astype(jnp.bfloat16), 4 * z).astype(f32)
        done.append(total.astype(jnp.bfloat16))
    placed = jnp.concatenate(done, axis=1)

    average = rows * devices * top / expert_count
    bias_next = bias + 2.0 / math.sqrt(average) * (average - counts[0, :expert_count])
    return (placed, bias_next)


def solution(mesh):
    placed = (
        P(("groups", "ep"), None),
        P(("groups", "ep"), None),
        P(("groups", "ep"), None),
        P(("groups", "ep")),
        P(),
        P(None, "ep"),
        P(None, "ep"),
        P("ep", None),
    )
    return jax.shard_map(
        per_device,
        mesh=mesh,
        in_specs=placed,
        out_specs=(P(("groups", "ep"), None), P("groups")),
        check_vma=False,
    )
```

```python
import math

import jax
import jax.numpy as jnp
from jax import lax
from jax.experimental import pallas as pl
from jax.experimental.pallas import tpu as pltpu
from jax.sharding import PartitionSpec as P

ROUTED_SCALE = 2.5
LANES = 128
VMEM = pl.BlockSpec(memory_space=pltpu.VMEM)
ANY = pl.BlockSpec(memory_space=pl.ANY)
HBM = pl.BlockSpec(memory_space=pltpu.HBM)
MIB = 1 << 20
SPARE = 3
LOTS = (2, 3, 1)


def divisor(total, want, step):
    best = step
    for size in range(step, min(total, want) + 1, step):
        if total % size == 0:
            best = size
    return best


def pack_rows(tokens, experts, gate_fixed, home_slot, expert_count):
    rows, width = tokens.shape
    top = experts.shape[1]
    extra = -(-2 * expert_count // LANES) * LANES

    def kernel(tok_hbm, exp_hbm, gate_hbm, home_hbm, out_ref, tok, exp, gate, home, sems):
        copies = [
            pltpu.make_async_copy(src, dst, sems.at[i])
            for i, (src, dst) in enumerate(((home_hbm, home), (exp_hbm, exp), (gate_hbm, gate), (tok_hbm, tok)))
        ]
        for copy in copies:
            copy.start()
        for copy in copies[:3]:
            copy.wait()
        row = lax.broadcasted_iota(jnp.int32, (rows, rows), 0)
        col = lax.broadcasted_iota(jnp.int32, (rows, rows), 1)
        placer = jnp.zeros((rows, rows), jnp.float32)
        for t in range(rows):
            placer = jnp.where((col == t) & (row == home[t]), 1.0, placer)
        placer = placer.astype(jnp.bfloat16)
        lane = lax.broadcasted_iota(jnp.int32, (rows, extra), 1)
        below = gate[...] - 1
        low, high = (below & 255) + 1, below >> 8
        meta = jnp.zeros((rows, extra), jnp.int32)
        for k in range(top):
            chosen = exp[:, k : k + 1]
            meta = jnp.where(lane == chosen, low[:, k : k + 1], meta)
            meta = jnp.where(lane == chosen + expert_count, high[:, k : k + 1], meta)
        out_ref[:, width:] = jnp.dot(
            placer, meta.astype(jnp.float32).astype(jnp.bfloat16), preferred_element_type=jnp.float32
        ).astype(jnp.bfloat16)
        copies[3].wait()
        out_ref[:, :width] = jnp.dot(
            placer, tok[...], preferred_element_type=jnp.float32
        ).astype(jnp.bfloat16)

    return pl.pallas_call(
        kernel,
        out_shape=jax.ShapeDtypeStruct((rows, width + extra), jnp.bfloat16),
        in_specs=[HBM] * 4,
        out_specs=VMEM,
        scratch_shapes=[
            pltpu.VMEM(tokens.shape, tokens.dtype),
            pltpu.VMEM(experts.shape, experts.dtype),
            pltpu.VMEM(gate_fixed.shape, gate_fixed.dtype),
            pltpu.SMEM(home_slot.shape, home_slot.dtype),
            pltpu.SemaphoreType.DMA((4,)),
        ],
        compiler_params=pltpu.CompilerParams(vmem_limit_bytes=4 * MIB),
        name="pack_rows",
    )(tokens, experts, gate_fixed, home_slot)


def fetch(w_gate, w_up, first, steps, cols, after, name):
    width = w_gate.shape[0]
    cuts = 4

    def kernel(*refs):
        gate_hbm, up_hbm, out, sems = refs[:2] + refs[-2:]
        size = width // cuts
        copies = []
        for s in range(steps):
            for c in range(cuts):
                part = pl.ds(c * size, size)
                for k, src in enumerate((gate_hbm, up_hbm)):
                    copies.append(
                        pltpu.make_async_copy(
                            src.at[part, pl.ds((first + s) * cols, cols)],
                            out.at[part, pl.ds((2 * s + k) * cols, cols)],
                            sems.at[len(copies)],
                        )
                    )
        for copy in copies:
            copy.start()
        for copy in copies:
            copy.wait()

    return pl.pallas_call(
        kernel,
        out_shape=pltpu.VMEM((width, 2 * steps * cols), w_gate.dtype),
        in_specs=[HBM] * 2 + [ANY] * len(after),
        out_specs=VMEM,
        scratch_shapes=[pltpu.SemaphoreType.DMA((2 * cuts * steps,))],
        compiler_params=pltpu.CompilerParams(vmem_limit_bytes=MIB),
        cost_estimate=pl.CostEstimate(
            flops=1024 * width * steps * cols, bytes_accessed=4 * width * steps * cols, transcendentals=0
        ),
        name=name,
    )(w_gate, w_up, *after)


def stack_rows(blocks):
    rows, width = blocks[0].shape
    count = len(blocks)

    def kernel(*refs):
        for b in range(count):
            refs[count][b * rows : (b + 1) * rows, :] = refs[b][...]

    return pl.pallas_call(
        kernel,
        out_shape=jax.ShapeDtypeStruct((count * rows, width), blocks[0].dtype),
        in_specs=[VMEM] * count,
        out_specs=VMEM,
        compiler_params=pltpu.CompilerParams(vmem_limit_bytes=(MIB if count <= 16 else 32 * MIB)),
        name="stack_rows",
    )(*blocks)


def add_rows(parts, rows):
    arrays = [array for terms in parts for array, _ in terms]
    widths = [terms[0][0].shape[1] for terms in parts]
    count = len(parts[0][0][1])

    def kernel(*refs):
        out, at, col = refs[-1], 0, 0
        for terms, width in zip(parts, widths):
            for b in range(count):
                total = None
                for t, (_, places) in enumerate(terms):
                    value = refs[at + t][places[b] * rows : (places[b] + 1) * rows, :].astype(jnp.float32)
                    total = value if total is None else total + value
                out[b * rows : (b + 1) * rows, col : col + width] = total.astype(jnp.bfloat16)
            at, col = at + len(terms), col + width

    small = max(array.shape[0] for array in arrays) <= 128
    if small:
        arrays = [pltpu.with_memory_space_constraint(array, pltpu.VMEM) for array in arrays]
    return pl.pallas_call(
        kernel,
        out_shape=jax.ShapeDtypeStruct((count * rows, sum(widths)), jnp.bfloat16),
        in_specs=[VMEM] * len(arrays),
        out_specs=VMEM,
        compiler_params=pltpu.CompilerParams(vmem_limit_bytes=2 * MIB if small else 48 * MIB),
        name="add_rows",
    )(*arrays)


def add_final(parts, rows):
    last = parts[0][-1][0]
    arrays = [array for terms in parts for array, _ in terms[:-1]] + [last]

    def kernel(*refs):
        at, col = 0, 0
        last_ref, out = refs[-2:]
        for terms in parts:
            width = terms[0][0].shape[1]
            total = last_ref[:, col : col + width].astype(jnp.float32)
            for t, (_, where) in enumerate(terms[:-1]):
                total = total + refs[at + t][where[0] * rows : (where[0] + 1) * rows, :].astype(jnp.float32)
            out[:, col : col + width] = total.astype(jnp.bfloat16)
            at, col = at + len(terms) - 1, col + width

    if max(array.shape[0] for array in arrays) <= 128:
        arrays = [pltpu.with_memory_space_constraint(array, pltpu.VMEM) for array in arrays]
    return pl.pallas_call(
        kernel,
        out_shape=jax.ShapeDtypeStruct(last.shape, jnp.bfloat16),
        in_specs=[VMEM] * len(arrays),
        out_specs=VMEM,
        compiler_params=pltpu.CompilerParams(vmem_limit_bytes=48 * MIB if parts[0][0][0].shape[0] > 128 else 2 * MIB),
        name="add_final",
    )(*arrays)


def expert_partials(near, other, fetched, up_cols, w_gate, w_up, w_down, expert_count, shards, pieces):
    half = near.shape[0]
    total = 2 * half
    width, units = w_gate.shape
    extra = near.shape[1] - width
    piece = width // pieces
    down_cols = divisor(piece, 2 * up_cols, LANES)
    up_steps, down_steps, per_piece = units // up_cols, width // down_cols, piece // down_cols
    sizes = [array.shape[1] // (2 * up_cols) for array in fetched]
    ready = sum(sizes)
    late = up_steps - ready
    stacked = width // units
    groups = -(-down_steps // stacked)
    lots = len(fetched)

    slot_of = [(lot, i) for lot, size in enumerate(sizes) for i in range(size)]
    order, streamed = [], 0
    for step in range(ready):
        order.append(step)
        if step % 2 == 1 and streamed < late:
            order.append(ready + streamed)
            streamed += 1
    order += range(ready + streamed, up_steps)

    def kernel(*refs):
        near_ref, other_ref = refs[:2]
        gate_hbm, up_hbm, down_hbm = refs[2 + lots : 5 + lots]
        at = 5 + lots
        outs, load_ref, lot_refs = refs[at : at + 2 * pieces], refs[at + 2 * pieces], refs[at + 2 * pieces + 1 :][:lots]
        x, meta, hidden, pool, up_sem, down_sem = refs[at + 2 * pieces + 1 + lots :]

        def slot_ref(slot, rows, cols):
            if slot is None:
                return pool.at[rows, cols]
            lot, i = slot
            return lot_refs[lot].at[rows, pl.ds(i * 2 * up_cols + cols.start, cols.size)]

        def up_copies(k, slot):
            cols = pl.ds((ready + k) * up_cols, up_cols)
            return [
                pltpu.make_async_copy(
                    src.at[:, cols], slot_ref(slot, pl.ds(0, width), pl.ds(i * up_cols, up_cols)), up_sem.at[k, i]
                )
                for i, src in enumerate((gate_hbm, up_hbm))
            ]

        def tile_ref(n, slot):
            return slot_ref(slot, pl.ds((n % stacked) * units, units), pl.ds(0, down_cols))

        def down_copy(n, slot):
            return pltpu.make_async_copy(
                down_hbm.at[:, pl.ds(n * down_cols, down_cols)], tile_ref(n, slot), down_sem.at[n]
            )

        loads = [("up", k) for k in range(late)] + [("down", g) for g in range(groups)]
        placed = {}

        def free(slot):
            if loads:
                kind, index = loads.pop(0)
                placed[kind, index] = slot
                if kind == "up":
                    for copy in up_copies(index, slot):
                        copy.start()
                else:
                    for n in range(index * stacked, min((index + 1) * stacked, down_steps)):
                        down_copy(n, slot).start()

        free(None)
        x[:half, :] = near_ref[:, :width]
        x[half:, :] = other_ref[:, :width]
        meta[:half, :] = near_ref[:, width:].astype(jnp.float32)
        meta[half:, :] = other_ref[:, width:].astype(jnp.float32)
        values = meta[...]
        lane = lax.broadcasted_iota(jnp.int32, (total, extra), 1)
        expert = lax.axis_index("ep") // shards
        is_low, is_high = lane < expert_count, (lane >= expert_count) & (lane < 2 * expert_count)
        scaled = jnp.where(is_high, 256.0 * values, jnp.where(is_low, values, 0.0))
        mine = (lane == expert) | (lane == expert + expert_count)
        own = jnp.sum(jnp.where(mine, scaled, 0.0), axis=1, keepdims=True)
        share = ROUTED_SCALE * own / jnp.sum(scaled, axis=1, keepdims=True)
        load_ref[...] = jnp.sum(jnp.where(is_low & (values > 0.0), 1.0, 0.0), axis=0, keepdims=True)

        for step in order:
            slot = slot_of[step] if step < ready else placed["up", step - ready]
            if step >= ready:
                for copy in up_copies(step - ready, slot):
                    copy.wait()
            tile = slot_ref(slot, pl.ds(0, width), pl.ds(0, 2 * up_cols))
            both = jnp.dot(x[...], tile[...], preferred_element_type=jnp.float32)
            gate, up = both[:, :up_cols], both[:, up_cols:]
            hidden[:, step * up_cols : (step + 1) * up_cols] = (gate / (1.0 + jnp.exp(-gate)) * up).astype(jnp.bfloat16)
            free(slot)
        for n in range(down_steps):
            slot = placed["down", n // stacked]
            down_copy(n, slot).wait()
            out = jnp.dot(hidden[...], tile_ref(n, slot)[...], preferred_element_type=jnp.float32)
            out = (out * share).astype(jnp.bfloat16)
            p, i = divmod(n, per_piece)
            outs[2 * p][:, i * down_cols : (i + 1) * down_cols] = out[:half]
            outs[2 * p + 1][:, i * down_cols : (i + 1) * down_cols] = out[half:]
            if n % stacked == stacked - 1:
                free(slot)

    kept = pltpu.VMEM if total <= 256 else jax.ShapeDtypeStruct
    shapes = [kept((half, piece), jnp.bfloat16)] * (2 * pieces)
    shapes.append(jax.ShapeDtypeStruct((1, extra), jnp.float32))
    shapes += [pltpu.VMEM(array.shape, array.dtype) for array in fetched]
    scratch = 2 * (total * (width + units + 2 * extra) + width * 2 * up_cols) + SPARE * MIB
    rows = [near, other]
    if total > 256:
        scratch += 4 * total * width
    else:
        rows = [pltpu.with_memory_space_constraint(array, pltpu.VMEM) for array in rows]
    lot_args = [pltpu.with_memory_space_constraint(array, pltpu.VMEM) for array in fetched]
    return pl.pallas_call(
        kernel,
        out_shape=shapes,
        in_specs=[VMEM] * (2 + lots) + [HBM] * 3,
        out_specs=[VMEM] * len(shapes),
        input_output_aliases={2 + lot: 2 * pieces + 1 + lot for lot in range(lots)},
        scratch_shapes=[
            pltpu.VMEM((total, width), jnp.bfloat16),
            pltpu.VMEM((total, extra), jnp.float32),
            pltpu.VMEM((total, units), jnp.bfloat16),
            pltpu.VMEM((width, 2 * up_cols), jnp.bfloat16),
            pltpu.SemaphoreType.DMA((max(1, late), 2)),
            pltpu.SemaphoreType.DMA((down_steps,)),
        ],
        compiler_params=pltpu.CompilerParams(vmem_limit_bytes=scratch),
        cost_estimate=pl.CostEstimate(
            flops=6 * total * width * units,
            bytes_accessed=6 * width * units,
            transcendentals=total * units,
        ),
        name="expert_partials",
    )(*rows, *lot_args, w_gate, w_up, w_down)[: 2 * pieces + 1]


def per_device(tokens, experts, gate_fixed, home_slot, bias, w_gate, w_up, w_down):
    tokens, experts, gate_fixed, home_slot, w_gate, w_up, w_down = (
        pltpu.with_memory_space_constraint(array, pltpu.HBM)
        for array in (tokens, experts, gate_fixed, home_slot, w_gate, w_up, w_down)
    )
    rows, width = tokens.shape
    units = w_gate.shape[1]
    top = experts.shape[1]
    expert_count = bias.shape[0]
    devices = lax.axis_size("ep")
    shards = devices // expert_count
    far = devices // 4
    up_cols = divisor(units, 256, LANES)

    def swap(value, mask):
        return lax.ppermute(value, "ep", [(i, i ^ mask) for i in range(devices)])

    lots, first = [], 0
    for most in LOTS:
        lots.append((first, min(most, units // up_cols - first)))
        first += lots[-1][1]

    def lot(k, after):
        if not lots[k][1]:
            return []
        return [fetch(w_gate, w_up, *lots[k], up_cols, after, "fetch_" + "abc"[k])]

    block = {0: pack_rows(tokens, experts, gate_fixed, home_slot, expert_count)}
    evens = [4 * z for z in range(2, far, 2)]
    for mask in evens + [4, 6, 2]:
        block[mask] = swap(block[0], mask)
    fetched = lot(0, [block[0]])
    *firsts, fetched = lax.optimization_barrier([block[mask] for mask in evens + [4, 6, 2]] + [fetched])
    block.update(zip(evens + [4, 6, 2], firsts))
    for even in evens:
        for mask in (4, 6, 2):
            block[even | mask] = swap(block[even], mask)
    fetched += lot(1, [block[even] for even in evens])
    seconds = [even | mask for even in evens for mask in (4, 6, 2)]
    *arrived, fetched = lax.optimization_barrier([block[mask] for mask in seconds] + [fetched])
    block.update(zip(seconds, arrived))
    bits = [2] + [4 << k for k in range((far - 1).bit_length())]
    masks = [0]
    for bit in reversed(bits):
        masks = masks + [mask | bit for mask in masks]
    near = stack_rows([block[mask] for mask in masks])
    other = swap(near, 1)
    fetched += lot(2, [near])

    *parts, counts = expert_partials(
        near, other, fetched, up_cols, w_gate, w_up, w_down, expert_count, shards, 2
    )

    places = {mask: i for i, mask in enumerate(masks)}
    halves = [[(parts[2 * p], places), (swap(parts[2 * p + 1], 1), places)] for p in range(2)]
    order = [bits, [bits[1], bits[0]] + bits[2:]]
    live = [list(masks), list(masks)]

    def chosen(p, want):
        return [(array, [where[mask] for mask in want]) for array, where in halves[p]]

    for k in range(len(bits) - 1):
        for p in range(2):
            bit = order[p][k]
            sent = [mask for mask in live[p] if mask & bit]
            live[p] = [mask for mask in live[p] if not mask & bit]
            came = swap(add_rows([chosen(p, sent)], rows), bit)
            halves[p].append((came, {mask ^ bit: i for i, mask in enumerate(sent)}))
    last = swap(add_rows([chosen(p, [bits[-1]]) for p in range(2)], rows), bits[-1])
    for p in range(2):
        halves[p].append((last, {0: 0}))
    placed = add_final([chosen(p, [0]) for p in range(2)], rows)

    average = rows * devices * top / expert_count
    bias_next = bias + 2.0 / math.sqrt(average) * (average - counts[0, :expert_count])
    return (placed, bias_next)


def solution(mesh):
    placed = (
        P(("groups", "ep"), None),
        P(("groups", "ep"), None),
        P(("groups", "ep"), None),
        P(("groups", "ep")),
        P(),
        P(None, "ep"),
        P(None, "ep"),
        P("ep", None),
    )
    return jax.shard_map(
        per_device,
        mesh=mesh,
        in_specs=placed,
        out_specs=(P(("groups", "ep"), None), P("groups")),
        check_vma=False,
    )
```

```python
import math

import jax
import jax.numpy as jnp
from jax import lax
from jax.experimental import pallas as pl
from jax.experimental.pallas import tpu as pltpu
from jax.sharding import PartitionSpec as P

ROUTED_SCALE = 2.5
LANES = 128
VMEM = pl.BlockSpec(memory_space=pltpu.VMEM)
ANY = pl.BlockSpec(memory_space=pl.ANY)
HBM = pl.BlockSpec(memory_space=pltpu.HBM)
MIB = 1 << 20
SPARE = 3
LOTS = (2, 3, 1)
AHEAD = 3
STEP_US = 1.0
LOAD_US = 2.2


def divisor(total, want, step):
    best = step
    for size in range(step, min(total, want) + 1, step):
        if total % size == 0:
            best = size
    return best


def pack_rows(tokens, experts, gate_fixed, home_slot, expert_count):
    rows, width = tokens.shape
    top = experts.shape[1]
    extra = -(-2 * expert_count // LANES) * LANES

    def kernel(tok_hbm, exp_hbm, gate_hbm, home_hbm, out_ref, tok, exp, gate, home, sems):
        copies = [
            pltpu.make_async_copy(src, dst, sems.at[i])
            for i, (src, dst) in enumerate(((home_hbm, home), (exp_hbm, exp), (gate_hbm, gate), (tok_hbm, tok)))
        ]
        for copy in copies:
            copy.start()
        for copy in copies[:3]:
            copy.wait()
        row = lax.broadcasted_iota(jnp.int32, (rows, rows), 0)
        col = lax.broadcasted_iota(jnp.int32, (rows, rows), 1)
        placer = jnp.zeros((rows, rows), jnp.float32)
        for t in range(rows):
            placer = jnp.where((col == t) & (row == home[t]), 1.0, placer)
        placer = placer.astype(jnp.bfloat16)
        lane = lax.broadcasted_iota(jnp.int32, (rows, extra), 1)
        below = gate[...] - 1
        low, high = (below & 255) + 1, below >> 8
        meta = jnp.zeros((rows, extra), jnp.int32)
        for k in range(top):
            chosen = exp[:, k : k + 1]
            meta = jnp.where(lane == chosen, low[:, k : k + 1], meta)
            meta = jnp.where(lane == chosen + expert_count, high[:, k : k + 1], meta)
        out_ref[:, width:] = jnp.dot(
            placer, meta.astype(jnp.float32).astype(jnp.bfloat16), preferred_element_type=jnp.float32
        ).astype(jnp.bfloat16)
        copies[3].wait()
        out_ref[:, :width] = jnp.dot(
            placer, tok[...], preferred_element_type=jnp.float32
        ).astype(jnp.bfloat16)

    return pl.pallas_call(
        kernel,
        out_shape=jax.ShapeDtypeStruct((rows, width + extra), jnp.bfloat16),
        in_specs=[HBM] * 4,
        out_specs=VMEM,
        scratch_shapes=[
            pltpu.VMEM(tokens.shape, tokens.dtype),
            pltpu.VMEM(experts.shape, experts.dtype),
            pltpu.VMEM(gate_fixed.shape, gate_fixed.dtype),
            pltpu.SMEM(home_slot.shape, home_slot.dtype),
            pltpu.SemaphoreType.DMA((4,)),
        ],
        compiler_params=pltpu.CompilerParams(vmem_limit_bytes=4 * MIB),
        name="pack_rows",
    )(tokens, experts, gate_fixed, home_slot)


def fetch(w_gate, w_up, first, steps, cols, after, name):
    width = w_gate.shape[0]
    cuts = 4

    def kernel(*refs):
        gate_hbm, up_hbm, out, sems = refs[:2] + refs[-2:]
        size = width // cuts
        copies = []
        for s in range(steps):
            for c in range(cuts):
                part = pl.ds(c * size, size)
                for k, src in enumerate((gate_hbm, up_hbm)):
                    copies.append(
                        pltpu.make_async_copy(
                            src.at[part, pl.ds((first + s) * cols, cols)],
                            out.at[part, pl.ds((2 * s + k) * cols, cols)],
                            sems.at[len(copies)],
                        )
                    )
        for copy in copies:
            copy.start()
        for copy in copies:
            copy.wait()

    return pl.pallas_call(
        kernel,
        out_shape=pltpu.VMEM((width, 2 * steps * cols), w_gate.dtype),
        in_specs=[HBM] * 2 + [ANY] * len(after),
        out_specs=VMEM,
        scratch_shapes=[pltpu.SemaphoreType.DMA((2 * cuts * steps,))],
        compiler_params=pltpu.CompilerParams(vmem_limit_bytes=MIB),
        cost_estimate=pl.CostEstimate(
            flops=1024 * width * steps * cols, bytes_accessed=4 * width * steps * cols, transcendentals=0
        ),
        name=name,
    )(w_gate, w_up, *after)


def stack_rows(pieces, rows):
    width = pieces[0][0].shape[1]
    count = len(pieces)

    def kernel(*refs):
        for b, (_, k) in enumerate(pieces):
            refs[count][b * rows : (b + 1) * rows, :] = refs[b][k * rows : (k + 1) * rows, :]

    return pl.pallas_call(
        kernel,
        out_shape=jax.ShapeDtypeStruct((count * rows, width), pieces[0][0].dtype),
        in_specs=[VMEM] * count,
        out_specs=VMEM,
        compiler_params=pltpu.CompilerParams(vmem_limit_bytes=(MIB if count <= 8 else 56 * MIB)),
        name="stack_rows",
    )(*[array for array, _ in pieces])


def add_rows(parts, rows):
    arrays = [array for terms in parts for array, _ in terms]
    widths = [terms[0][0].shape[1] for terms in parts]
    count = len(parts[0][0][1])

    def kernel(*refs):
        out, at, col = refs[-1], 0, 0
        for terms, width in zip(parts, widths):
            for b in range(count):
                total = None
                for t, (_, places) in enumerate(terms):
                    value = refs[at + t][places[b] * rows : (places[b] + 1) * rows, :].astype(jnp.float32)
                    total = value if total is None else total + value
                out[b * rows : (b + 1) * rows, col : col + width] = total.astype(jnp.bfloat16)
            at, col = at + len(terms), col + width

    small = max(array.shape[0] for array in arrays) <= 128
    if small:
        arrays = [pltpu.with_memory_space_constraint(array, pltpu.VMEM) for array in arrays]
    return pl.pallas_call(
        kernel,
        out_shape=jax.ShapeDtypeStruct((count * rows, sum(widths)), jnp.bfloat16),
        in_specs=[VMEM] * len(arrays),
        out_specs=VMEM,
        compiler_params=pltpu.CompilerParams(vmem_limit_bytes=2 * MIB if small else 48 * MIB),
        name="add_rows",
    )(*arrays)


def add_final(parts, rows):
    last = parts[0][-1][0]
    arrays = [array for terms in parts for array, _ in terms[:-1]] + [last]

    def kernel(*refs):
        at, col = 0, 0
        last_ref, out = refs[-2:]
        for terms in parts:
            width = terms[0][0].shape[1]
            total = last_ref[:, col : col + width].astype(jnp.float32)
            for t, (_, where) in enumerate(terms[:-1]):
                total = total + refs[at + t][where[0] * rows : (where[0] + 1) * rows, :].astype(jnp.float32)
            out[:, col : col + width] = total.astype(jnp.bfloat16)
            at, col = at + len(terms) - 1, col + width

    if max(array.shape[0] for array in arrays) <= 128:
        arrays = [pltpu.with_memory_space_constraint(array, pltpu.VMEM) for array in arrays]
    return pl.pallas_call(
        kernel,
        out_shape=jax.ShapeDtypeStruct(last.shape, jnp.bfloat16),
        in_specs=[VMEM] * len(arrays),
        out_specs=VMEM,
        compiler_params=pltpu.CompilerParams(vmem_limit_bytes=48 * MIB if parts[0][0][0].shape[0] > 128 else 2 * MIB),
        name="add_final",
    )(*arrays)


def expert_partials(near, other, fetched, up_cols, w_gate, w_up, w_down, expert_count, shards, pieces):
    half = near.shape[0]
    total = 2 * half
    width, units = w_gate.shape
    extra = near.shape[1] - width
    piece = width // pieces
    down_cols = divisor(piece, 2 * up_cols, LANES)
    up_steps, down_steps, per_piece = units // up_cols, width // down_cols, piece // down_cols
    sizes = [array.shape[1] // (2 * up_cols) for array in fetched]
    ready = sum(sizes)
    late = up_steps - ready
    stacked = width // units
    groups = -(-down_steps // stacked)
    lots = len(fetched)

    slot_of = [(lot, i) for lot, size in enumerate(sizes) for i in range(size)]
    order, streamed = [], 0
    for step in range(ready):
        order.append(("up", step))
        if step % 2 == 1 and streamed < late:
            order.append(("up", ready + streamed))
            streamed += 1
    order += [("up", step) for step in range(ready + streamed, up_steps)]
    order += [("down", g) for g in range(groups)]

    loads = [unit for unit in order if unit[0] == "down" or unit[1] >= ready]
    before, behind, placed = {}, {}, {}
    flying, open_slots, landed, now, wire = [], [None], {}, 0.0, 0.0
    for at, unit in enumerate([None] + order):
        todo = before.setdefault(unit, [])
        if unit in loads and unit in flying:
            todo.append(("wait", unit))
            now = max(now, landed[unit])
            flying.remove(unit)
        if unit is not None:
            now += STEP_US if unit[0] == "up" else STEP_US / 2
            open_slots.append(slot_of[unit[1]] if unit[0] == "up" and unit[1] < ready else placed[unit])
        todo = behind.setdefault(unit, [])
        for load in [load for load in flying if landed[load] <= now]:
            todo.append(("wait", load))
            flying.remove(load)
        while loads and len(placed) < len(loads) and open_slots and len(flying) < AHEAD:
            load = loads[len(placed)]
            placed[load] = open_slots.pop(0)
            wire = max(wire, now) + LOAD_US
            landed[load] = wire + 0.7
            flying.append(load)
            todo.append(("start", load))
    assert len(placed) == len(loads)

    def kernel(*refs):
        near_ref, other_ref = refs[:2]
        gate_hbm, up_hbm, down_hbm = refs[2 + lots : 5 + lots]
        at = 5 + lots
        outs, load_ref, lot_refs = refs[at : at + 2 * pieces], refs[at + 2 * pieces], refs[at + 2 * pieces + 1 :][:lots]
        x, meta, hidden, pool, up_sem, down_sem = refs[at + 2 * pieces + 1 + lots :]

        def slot_ref(slot, rows, cols):
            if slot is None:
                return pool.at[rows, cols]
            lot, i = slot
            return lot_refs[lot].at[rows, pl.ds(i * 2 * up_cols + cols.start, cols.size)]

        def tile_ref(n):
            slot = placed["down", n // stacked]
            return slot_ref(slot, pl.ds((n % stacked) * units, units), pl.ds(0, down_cols))

        def copies(load):
            kind, index = load
            if kind == "up":
                cols = pl.ds(index * up_cols, up_cols)
                for i, src in enumerate((gate_hbm, up_hbm)):
                    out = slot_ref(placed[load], pl.ds(0, width), pl.ds(i * up_cols, up_cols))
                    yield pltpu.make_async_copy(src.at[:, cols], out, up_sem.at[index - ready, i])
            else:
                for n in range(index * stacked, min((index + 1) * stacked, down_steps)):
                    src = down_hbm.at[:, pl.ds(n * down_cols, down_cols)]
                    yield pltpu.make_async_copy(src, tile_ref(n), down_sem.at[n])

        def run(todo):
            for what, load in todo:
                for copy in copies(load):
                    copy.start() if what == "start" else copy.wait()

        run(behind[None])
        x[:half, :] = near_ref[:, :width]
        x[half:, :] = other_ref[:, :width]
        meta[:half, :] = near_ref[:, width:].astype(jnp.float32)
        meta[half:, :] = other_ref[:, width:].astype(jnp.float32)
        values = meta[...]
        lane = lax.broadcasted_iota(jnp.int32, (total, extra), 1)
        expert = lax.axis_index("ep") // shards
        is_low, is_high = lane < expert_count, (lane >= expert_count) & (lane < 2 * expert_count)
        scaled = jnp.where(is_high, 256.0 * values, jnp.where(is_low, values, 0.0))
        mine = (lane == expert) | (lane == expert + expert_count)
        own = jnp.sum(jnp.where(mine, scaled, 0.0), axis=1, keepdims=True)
        share = ROUTED_SCALE * own / jnp.sum(scaled, axis=1, keepdims=True)
        load_ref[...] = jnp.sum(jnp.where(is_low & (values > 0.0), 1.0, 0.0), axis=0, keepdims=True)

        for unit in order:
            kind, index = unit
            run(before[unit])
            if kind == "up":
                slot = slot_of[index] if index < ready else placed[unit]
                tile = slot_ref(slot, pl.ds(0, width), pl.ds(0, 2 * up_cols))
                both = jnp.dot(x[...], tile[...], preferred_element_type=jnp.float32)
                gate, up = both[:, :up_cols], both[:, up_cols:]
                hidden[:, index * up_cols : (index + 1) * up_cols] = (gate / (1.0 + jnp.exp(-gate)) * up).astype(
                    jnp.bfloat16
                )
            else:
                for n in range(index * stacked, min((index + 1) * stacked, down_steps)):
                    out = jnp.dot(hidden[...], tile_ref(n)[...], preferred_element_type=jnp.float32)
                    out = (out * share).astype(jnp.bfloat16)
                    p, i = divmod(n, per_piece)
                    outs[2 * p][:, i * down_cols : (i + 1) * down_cols] = out[:half]
                    outs[2 * p + 1][:, i * down_cols : (i + 1) * down_cols] = out[half:]
            run(behind[unit])

    kept = pltpu.VMEM if total <= 256 else jax.ShapeDtypeStruct
    shapes = [kept((half, piece), jnp.bfloat16)] * (2 * pieces)
    shapes.append(jax.ShapeDtypeStruct((1, extra), jnp.float32))
    shapes += [pltpu.VMEM(array.shape, array.dtype) for array in fetched]
    scratch = 2 * (total * (width + units + 2 * extra) + width * 2 * up_cols) + SPARE * MIB
    rows = [near, other]
    if total > 256:
        scratch += 4 * total * width
    else:
        rows = [pltpu.with_memory_space_constraint(array, pltpu.VMEM) for array in rows]
    lot_args = [pltpu.with_memory_space_constraint(array, pltpu.VMEM) for array in fetched]
    return pl.pallas_call(
        kernel,
        out_shape=shapes,
        in_specs=[VMEM] * (2 + lots) + [HBM] * 3,
        out_specs=[VMEM] * len(shapes),
        input_output_aliases={2 + lot: 2 * pieces + 1 + lot for lot in range(lots)},
        scratch_shapes=[
            pltpu.VMEM((total, width), jnp.bfloat16),
            pltpu.VMEM((total, extra), jnp.float32),
            pltpu.VMEM((total, units), jnp.bfloat16),
            pltpu.VMEM((width, 2 * up_cols), jnp.bfloat16),
            pltpu.SemaphoreType.DMA((max(1, late), 2)),
            pltpu.SemaphoreType.DMA((down_steps,)),
        ],
        compiler_params=pltpu.CompilerParams(vmem_limit_bytes=scratch),
        cost_estimate=pl.CostEstimate(
            flops=6 * total * width * units,
            bytes_accessed=6 * width * units,
            transcendentals=total * units,
        ),
        name="expert_partials",
    )(*rows, *lot_args, w_gate, w_up, w_down)[: 2 * pieces + 1]


def per_device(tokens, experts, gate_fixed, home_slot, bias, w_gate, w_up, w_down):
    tokens, experts, gate_fixed, home_slot, w_gate, w_up, w_down = (
        pltpu.with_memory_space_constraint(array, pltpu.HBM)
        for array in (tokens, experts, gate_fixed, home_slot, w_gate, w_up, w_down)
    )
    rows, width = tokens.shape
    units = w_gate.shape[1]
    top = experts.shape[1]
    expert_count = bias.shape[0]
    devices = lax.axis_size("ep")
    shards = devices // expert_count
    far = devices // 4
    up_cols = divisor(units, 256, LANES)

    def swap(value, mask):
        return lax.ppermute(value, "ep", [(i, i ^ mask) for i in range(devices)])

    lots, first = [], 0
    for most in LOTS:
        lots.append((first, min(most, units // up_cols - first)))
        first += lots[-1][1]

    def lot(k, after):
        if not lots[k][1]:
            return []
        return [fetch(w_gate, w_up, *lots[k], up_cols, after, "fetch_" + "abc"[k])]

    block = {0: pack_rows(tokens, experts, gate_fixed, home_slot, expert_count)}
    evens = [4 * z for z in range(2, far, 2)]
    firsts = [2, 4] + evens
    for mask in firsts:
        block[mask] = swap(block[0], mask)
    fetched = lot(0, [block[0]])
    *arrived, fetched = lax.optimization_barrier([block[mask] for mask in firsts] + [fetched])
    block.update(zip(firsts, arrived))
    for even in evens:
        for mask in (4, 6):
            block[even | mask] = swap(block[even], mask)
    pair = [4] + evens
    across = swap(stack_rows([(block[mask], 0) for mask in pair], rows), 2)
    fetched += lot(1, [block[even] for even in evens])
    seconds = [even | mask for even in evens for mask in (4, 6)]
    *arrived, across, fetched = lax.optimization_barrier([block[mask] for mask in seconds] + [across, fetched])
    block.update(zip(seconds, arrived))
    piece = {mask: (array, 0) for mask, array in block.items()}
    piece.update({mask | 2: (across, i) for i, mask in enumerate(pair)})
    bits = [2] + [4 << k for k in range((far - 1).bit_length())]
    masks = [0]
    for bit in reversed(bits):
        masks = masks + [mask | bit for mask in masks]
    near = stack_rows([piece[mask] for mask in masks], rows)
    other = swap(near, 1)
    fetched += lot(2, [near])

    *parts, counts = expert_partials(
        near, other, fetched, up_cols, w_gate, w_up, w_down, expert_count, shards, 2
    )

    places = {mask: i for i, mask in enumerate(masks)}
    halves = [[(parts[2 * p], places), (swap(parts[2 * p + 1], 1), places)] for p in range(2)]
    order = [bits, [bits[1], bits[0]] + bits[2:]]
    live = [list(masks), list(masks)]

    def chosen(p, want):
        return [(array, [where[mask] for mask in want]) for array, where in halves[p]]

    for k in range(len(bits) - 1):
        for p in range(2):
            bit = order[p][k]
            sent = [mask for mask in live[p] if mask & bit]
            live[p] = [mask for mask in live[p] if not mask & bit]
            came = swap(add_rows([chosen(p, sent)], rows), bit)
            halves[p].append((came, {mask ^ bit: i for i, mask in enumerate(sent)}))
    last = swap(add_rows([chosen(p, [bits[-1]]) for p in range(2)], rows), bits[-1])
    for p in range(2):
        halves[p].append((last, {0: 0}))
    placed = add_final([chosen(p, [0]) for p in range(2)], rows)

    average = rows * devices * top / expert_count
    bias_next = bias + 2.0 / math.sqrt(average) * (average - counts[0, :expert_count])
    return (placed, bias_next)


def solution(mesh):
    placed = (
        P(("groups", "ep"), None),
        P(("groups", "ep"), None),
        P(("groups", "ep"), None),
        P(("groups", "ep")),
        P(),
        P(None, "ep"),
        P(None, "ep"),
        P("ep", None),
    )
    return jax.shard_map(
        per_device,
        mesh=mesh,
        in_specs=placed,
        out_specs=(P(("groups", "ep"), None), P("groups")),
        check_vma=False,
    )
```

```python
import math

import jax
import jax.numpy as jnp
from jax import lax
from jax.experimental import pallas as pl
from jax.experimental.pallas import tpu as pltpu
from jax.sharding import PartitionSpec as P

ROUTED_SCALE = 2.5
LANES = 128
VMEM = pl.BlockSpec(memory_space=pltpu.VMEM)
ANY = pl.BlockSpec(memory_space=pl.ANY)
HBM = pl.BlockSpec(memory_space=pltpu.HBM)
MIB = 1 << 20
SPARE = 3
LOTS = (2, 3, 1)
AHEAD = 3
STEP_US = 1.0
LOAD_US = 2.2


def divisor(total, want, step):
    best = step
    for size in range(step, min(total, want) + 1, step):
        if total % size == 0:
            best = size
    return best


def pack_rows(tokens, experts, gate_fixed, home_slot, expert_count):
    rows, width = tokens.shape
    top = experts.shape[1]
    extra = -(-2 * expert_count // LANES) * LANES

    def kernel(tok_hbm, exp_hbm, gate_hbm, home_hbm, out_ref, tok, exp, gate, home, sems):
        copies = [
            pltpu.make_async_copy(src, dst, sems.at[i])
            for i, (src, dst) in enumerate(((home_hbm, home), (exp_hbm, exp), (gate_hbm, gate), (tok_hbm, tok)))
        ]
        for copy in copies:
            copy.start()
        for copy in copies[:3]:
            copy.wait()
        row = lax.broadcasted_iota(jnp.int32, (rows, rows), 0)
        col = lax.broadcasted_iota(jnp.int32, (rows, rows), 1)
        placer = jnp.zeros((rows, rows), jnp.float32)
        for t in range(rows):
            placer = jnp.where((col == t) & (row == home[t]), 1.0, placer)
        placer = placer.astype(jnp.bfloat16)
        lane = lax.broadcasted_iota(jnp.int32, (rows, extra), 1)
        below = gate[...] - 1
        low, high = (below & 255) + 1, below >> 8
        meta = jnp.zeros((rows, extra), jnp.int32)
        for k in range(top):
            chosen = exp[:, k : k + 1]
            meta = jnp.where(lane == chosen, low[:, k : k + 1], meta)
            meta = jnp.where(lane == chosen + expert_count, high[:, k : k + 1], meta)
        out_ref[:, width:] = jnp.dot(
            placer, meta.astype(jnp.float32).astype(jnp.bfloat16), preferred_element_type=jnp.float32
        ).astype(jnp.bfloat16)
        copies[3].wait()
        out_ref[:, :width] = jnp.dot(
            placer, tok[...], preferred_element_type=jnp.float32
        ).astype(jnp.bfloat16)

    return pl.pallas_call(
        kernel,
        out_shape=jax.ShapeDtypeStruct((rows, width + extra), jnp.bfloat16),
        in_specs=[HBM] * 4,
        out_specs=VMEM,
        scratch_shapes=[
            pltpu.VMEM(tokens.shape, tokens.dtype),
            pltpu.VMEM(experts.shape, experts.dtype),
            pltpu.VMEM(gate_fixed.shape, gate_fixed.dtype),
            pltpu.SMEM(home_slot.shape, home_slot.dtype),
            pltpu.SemaphoreType.DMA((4,)),
        ],
        compiler_params=pltpu.CompilerParams(vmem_limit_bytes=4 * MIB),
        name="pack_rows",
    )(tokens, experts, gate_fixed, home_slot)


def fetch(w_gate, w_up, first, steps, cols, after, name):
    width = w_gate.shape[0]

    def kernel(*refs):
        gate_hbm, up_hbm, out, sems = refs[:2] + refs[-2:]
        copies = []
        for s in range(steps):
            for k, src in enumerate((gate_hbm, up_hbm)):
                copies.append(
                    pltpu.make_async_copy(
                        src.at[:, pl.ds((first + s) * cols, cols)],
                        out.at[:, pl.ds((2 * s + k) * cols, cols)],
                        sems.at[len(copies)],
                    )
                )
        for copy in copies:
            copy.start()
        for copy in copies:
            copy.wait()

    return pl.pallas_call(
        kernel,
        out_shape=pltpu.VMEM((width, 2 * steps * cols), w_gate.dtype),
        in_specs=[HBM] * 2 + [ANY] * len(after),
        out_specs=VMEM,
        scratch_shapes=[pltpu.SemaphoreType.DMA((2 * steps,))],
        compiler_params=pltpu.CompilerParams(vmem_limit_bytes=MIB),
        cost_estimate=pl.CostEstimate(
            flops=1024 * width * steps * cols, bytes_accessed=4 * width * steps * cols, transcendentals=0
        ),
        name=name,
    )(w_gate, w_up, *after)


def stack_rows(pieces, rows):
    width = pieces[0][0].shape[1]
    count = len(pieces)

    def kernel(*refs):
        for b, (_, k) in enumerate(pieces):
            refs[count][b * rows : (b + 1) * rows, :] = refs[b][k * rows : (k + 1) * rows, :]

    return pl.pallas_call(
        kernel,
        out_shape=jax.ShapeDtypeStruct((count * rows, width), pieces[0][0].dtype),
        in_specs=[VMEM] * count,
        out_specs=VMEM,
        compiler_params=pltpu.CompilerParams(vmem_limit_bytes=(MIB if count <= 8 else 56 * MIB)),
        name="stack_rows",
    )(*[array for array, _ in pieces])


def add_rows(parts, rows):
    arrays = [array for terms in parts for array, _ in terms]
    widths = [terms[0][0].shape[1] for terms in parts]
    count = len(parts[0][0][1])

    def kernel(*refs):
        out, at, col = refs[-1], 0, 0
        for terms, width in zip(parts, widths):
            for b in range(count):
                total = None
                for t, (_, places) in enumerate(terms):
                    value = refs[at + t][places[b] * rows : (places[b] + 1) * rows, :].astype(jnp.float32)
                    total = value if total is None else total + value
                out[b * rows : (b + 1) * rows, col : col + width] = total.astype(jnp.bfloat16)
            at, col = at + len(terms), col + width

    small = max(array.shape[0] for array in arrays) <= 128
    if small:
        arrays = [pltpu.with_memory_space_constraint(array, pltpu.VMEM) for array in arrays]
    return pl.pallas_call(
        kernel,
        out_shape=jax.ShapeDtypeStruct((count * rows, sum(widths)), jnp.bfloat16),
        in_specs=[VMEM] * len(arrays),
        out_specs=VMEM,
        compiler_params=pltpu.CompilerParams(vmem_limit_bytes=2 * MIB if small else 48 * MIB),
        name="add_rows",
    )(*arrays)


def add_final(parts, rows):
    last = parts[0][-1][0]
    arrays = [array for terms in parts for array, _ in terms[:-1]] + [last]

    def kernel(*refs):
        at, col = 0, 0
        last_ref, out = refs[-2:]
        for terms in parts:
            width = terms[0][0].shape[1]
            total = last_ref[:, col : col + width].astype(jnp.float32)
            for t, (_, where) in enumerate(terms[:-1]):
                total = total + refs[at + t][where[0] * rows : (where[0] + 1) * rows, :].astype(jnp.float32)
            out[:, col : col + width] = total.astype(jnp.bfloat16)
            at, col = at + len(terms) - 1, col + width

    if max(array.shape[0] for array in arrays) <= 128:
        arrays = [pltpu.with_memory_space_constraint(array, pltpu.VMEM) for array in arrays]
    return pl.pallas_call(
        kernel,
        out_shape=jax.ShapeDtypeStruct(last.shape, jnp.bfloat16),
        in_specs=[VMEM] * len(arrays),
        out_specs=VMEM,
        compiler_params=pltpu.CompilerParams(vmem_limit_bytes=48 * MIB if parts[0][0][0].shape[0] > 128 else 2 * MIB),
        name="add_final",
    )(*arrays)


def expert_partials(near, other, fetched, up_cols, w_gate, w_up, w_down, expert_count, shards, pieces):
    half = near.shape[0]
    total = 2 * half
    width, units = w_gate.shape
    extra = near.shape[1] - width
    piece = width // pieces
    down_cols = divisor(piece, 2 * up_cols, LANES)
    up_steps, down_steps, per_piece = units // up_cols, width // down_cols, piece // down_cols
    sizes = [array.shape[1] // (2 * up_cols) for array in fetched]
    ready = sum(sizes)
    late = up_steps - ready
    stacked = width // units
    groups = -(-down_steps // stacked)
    lots = len(fetched)

    slot_of = [(lot, i) for lot, size in enumerate(sizes) for i in range(size)]
    order, streamed = [], 0
    for step in range(ready):
        order.append(("up", step))
        if step % 2 == 1 and streamed < late:
            order.append(("up", ready + streamed))
            streamed += 1
    order += [("up", step) for step in range(ready + streamed, up_steps)]
    order += [("down", g) for g in range(groups)]

    loads = [unit for unit in order if unit[0] == "down" or unit[1] >= ready]
    before, behind, placed = {}, {}, {}
    flying, open_slots, landed, now, wire = [], [None], {}, 0.0, 0.0
    for at, unit in enumerate([None] + order):
        todo = before.setdefault(unit, [])
        if unit in loads and unit in flying:
            todo.append(("wait", unit))
            now = max(now, landed[unit])
            flying.remove(unit)
        if unit is not None:
            now += STEP_US if unit[0] == "up" else STEP_US / 2
            open_slots.append(slot_of[unit[1]] if unit[0] == "up" and unit[1] < ready else placed[unit])
        todo = behind.setdefault(unit, [])
        for load in [load for load in flying if landed[load] <= now]:
            todo.append(("wait", load))
            flying.remove(load)
        while loads and len(placed) < len(loads) and open_slots and len(flying) < AHEAD:
            load = loads[len(placed)]
            placed[load] = open_slots.pop(0)
            wire = max(wire, now) + LOAD_US
            landed[load] = wire + 0.7
            flying.append(load)
            todo.append(("start", load))
    assert len(placed) == len(loads)

    def kernel(*refs):
        near_ref, other_ref = refs[:2]
        gate_hbm, up_hbm, down_hbm = refs[2 + lots : 5 + lots]
        at = 5 + lots
        outs, load_ref, lot_refs = refs[at : at + 2 * pieces], refs[at + 2 * pieces], refs[at + 2 * pieces + 1 :][:lots]
        x, meta, hidden, pool, up_sem, down_sem = refs[at + 2 * pieces + 1 + lots :]

        def slot_ref(slot, rows, cols):
            if slot is None:
                return pool.at[rows, cols]
            lot, i = slot
            return lot_refs[lot].at[rows, pl.ds(i * 2 * up_cols + cols.start, cols.size)]

        def tile_ref(n):
            slot = placed["down", n // stacked]
            return slot_ref(slot, pl.ds((n % stacked) * units, units), pl.ds(0, down_cols))

        def copies(load):
            kind, index = load
            if kind == "up":
                cols = pl.ds(index * up_cols, up_cols)
                for i, src in enumerate((gate_hbm, up_hbm)):
                    out = slot_ref(placed[load], pl.ds(0, width), pl.ds(i * up_cols, up_cols))
                    yield pltpu.make_async_copy(src.at[:, cols], out, up_sem.at[index - ready, i])
            else:
                for n in range(index * stacked, min((index + 1) * stacked, down_steps)):
                    src = down_hbm.at[:, pl.ds(n * down_cols, down_cols)]
                    yield pltpu.make_async_copy(src, tile_ref(n), down_sem.at[n])

        def run(todo):
            for what, load in todo:
                for copy in copies(load):
                    copy.start() if what == "start" else copy.wait()

        run(behind[None])
        x[:half, :] = near_ref[:, :width]
        x[half:, :] = other_ref[:, :width]
        meta[:half, :] = near_ref[:, width:].astype(jnp.float32)
        meta[half:, :] = other_ref[:, width:].astype(jnp.float32)
        values = meta[...]
        lane = lax.broadcasted_iota(jnp.int32, (total, extra), 1)
        expert = lax.axis_index("ep") // shards
        is_low, is_high = lane < expert_count, (lane >= expert_count) & (lane < 2 * expert_count)
        scaled = jnp.where(is_high, 256.0 * values, jnp.where(is_low, values, 0.0))
        mine = (lane == expert) | (lane == expert + expert_count)
        own = jnp.sum(jnp.where(mine, scaled, 0.0), axis=1, keepdims=True)
        share = ROUTED_SCALE * own / jnp.sum(scaled, axis=1, keepdims=True)
        load_ref[...] = jnp.sum(jnp.where(is_low & (values > 0.0), 1.0, 0.0), axis=0, keepdims=True)

        for unit in order:
            kind, index = unit
            run(before[unit])
            if kind == "up":
                slot = slot_of[index] if index < ready else placed[unit]
                tile = slot_ref(slot, pl.ds(0, width), pl.ds(0, 2 * up_cols))
                both = jnp.dot(x[...], tile[...], preferred_element_type=jnp.float32)
                gate, up = both[:, :up_cols], both[:, up_cols:]
                hidden[:, index * up_cols : (index + 1) * up_cols] = (gate / (1.0 + jnp.exp(-gate)) * up).astype(
                    jnp.bfloat16
                )
            else:
                for n in range(index * stacked, min((index + 1) * stacked, down_steps)):
                    out = jnp.dot(hidden[...], tile_ref(n)[...], preferred_element_type=jnp.float32)
                    out = (out * share).astype(jnp.bfloat16)
                    p, i = divmod(n, per_piece)
                    outs[2 * p][:, i * down_cols : (i + 1) * down_cols] = out[:half]
                    outs[2 * p + 1][:, i * down_cols : (i + 1) * down_cols] = out[half:]
            run(behind[unit])

    kept = pltpu.VMEM if total <= 256 else jax.ShapeDtypeStruct
    shapes = [kept((half, piece), jnp.bfloat16)] * (2 * pieces)
    shapes.append(jax.ShapeDtypeStruct((1, extra), jnp.float32))
    shapes += [pltpu.VMEM(array.shape, array.dtype) for array in fetched]
    scratch = 2 * (total * (width + units + 2 * extra) + width * 2 * up_cols) + SPARE * MIB
    rows = [near, other]
    if total > 256:
        scratch += 4 * total * width
    else:
        rows = [pltpu.with_memory_space_constraint(array, pltpu.VMEM) for array in rows]
    lot_args = [pltpu.with_memory_space_constraint(array, pltpu.VMEM) for array in fetched]
    return pl.pallas_call(
        kernel,
        out_shape=shapes,
        in_specs=[VMEM] * (2 + lots) + [HBM] * 3,
        out_specs=[VMEM] * len(shapes),
        input_output_aliases={2 + lot: 2 * pieces + 1 + lot for lot in range(lots)},
        scratch_shapes=[
            pltpu.VMEM((total, width), jnp.bfloat16),
            pltpu.VMEM((total, extra), jnp.float32),
            pltpu.VMEM((total, units), jnp.bfloat16),
            pltpu.VMEM((width, 2 * up_cols), jnp.bfloat16),
            pltpu.SemaphoreType.DMA((max(1, late), 2)),
            pltpu.SemaphoreType.DMA((down_steps,)),
        ],
        compiler_params=pltpu.CompilerParams(vmem_limit_bytes=scratch),
        cost_estimate=pl.CostEstimate(
            flops=6 * total * width * units,
            bytes_accessed=6 * width * units,
            transcendentals=total * units,
        ),
        name="expert_partials",
    )(*rows, *lot_args, w_gate, w_up, w_down)[: 2 * pieces + 1]


def per_device(tokens, experts, gate_fixed, home_slot, bias, w_gate, w_up, w_down):
    tokens, experts, gate_fixed, home_slot, w_gate, w_up, w_down = (
        pltpu.with_memory_space_constraint(array, pltpu.HBM)
        for array in (tokens, experts, gate_fixed, home_slot, w_gate, w_up, w_down)
    )
    rows, width = tokens.shape
    units = w_gate.shape[1]
    top = experts.shape[1]
    expert_count = bias.shape[0]
    devices = lax.axis_size("ep")
    shards = devices // expert_count
    far = devices // 4
    up_cols = divisor(units, 256, LANES)

    def swap(value, mask):
        return lax.ppermute(value, "ep", [(i, i ^ mask) for i in range(devices)])

    lots, first = [], 0
    for most in LOTS:
        lots.append((first, min(most, units // up_cols - first)))
        first += lots[-1][1]

    def lot(k, after):
        if not lots[k][1]:
            return []
        return [fetch(w_gate, w_up, *lots[k], up_cols, after, "fetch_" + "abc"[k])]

    block = {0: pack_rows(tokens, experts, gate_fixed, home_slot, expert_count)}
    evens = [4 * z for z in range(2, far, 2)]
    firsts = [2, 4] + evens
    for mask in firsts:
        block[mask] = swap(block[0], mask)
    fetched = lot(0, [block[0]])
    *arrived, fetched = lax.optimization_barrier([block[mask] for mask in firsts] + [fetched])
    block.update(zip(firsts, arrived))
    for even in evens:
        for mask in (4, 6):
            block[even | mask] = swap(block[even], mask)
    pair = [4] + evens
    across = swap(stack_rows([(block[mask], 0) for mask in pair], rows), 2)
    fetched += lot(1, [block[even] for even in evens])
    seconds = [even | mask for even in evens for mask in (4, 6)]
    *arrived, across, fetched = lax.optimization_barrier([block[mask] for mask in seconds] + [across, fetched])
    block.update(zip(seconds, arrived))
    piece = {mask: (array, 0) for mask, array in block.items()}
    piece.update({mask | 2: (across, i) for i, mask in enumerate(pair)})
    bits = [2] + [4 << k for k in range((far - 1).bit_length())]
    masks = [0]
    for bit in reversed(bits):
        masks = masks + [mask | bit for mask in masks]
    near = stack_rows([piece[mask] for mask in masks], rows)
    other = swap(near, 1)
    fetched += lot(2, [near])

    *parts, counts = expert_partials(
        near, other, fetched, up_cols, w_gate, w_up, w_down, expert_count, shards, 2
    )

    places = {mask: i for i, mask in enumerate(masks)}
    halves = [[(parts[2 * p], places), (swap(parts[2 * p + 1], 1), places)] for p in range(2)]
    order = [bits, [bits[1], bits[0]] + bits[2:]]
    live = [list(masks), list(masks)]

    def chosen(p, want):
        return [(array, [where[mask] for mask in want]) for array, where in halves[p]]

    for k in range(len(bits) - 1):
        for p in range(2):
            bit = order[p][k]
            sent = [mask for mask in live[p] if mask & bit]
            live[p] = [mask for mask in live[p] if not mask & bit]
            came = swap(add_rows([chosen(p, sent)], rows), bit)
            halves[p].append((came, {mask ^ bit: i for i, mask in enumerate(sent)}))
    last = swap(add_rows([chosen(p, [bits[-1]]) for p in range(2)], rows), bits[-1])
    for p in range(2):
        halves[p].append((last, {0: 0}))
    placed = add_final([chosen(p, [0]) for p in range(2)], rows)

    average = rows * devices * top / expert_count
    bias_next = bias + 2.0 / math.sqrt(average) * (average - counts[0, :expert_count])
    return (placed, bias_next)


def solution(mesh):
    placed = (
        P(("groups", "ep"), None),
        P(("groups", "ep"), None),
        P(("groups", "ep"), None),
        P(("groups", "ep")),
        P(),
        P(None, "ep"),
        P(None, "ep"),
        P("ep", None),
    )
    return jax.shard_map(
        per_device,
        mesh=mesh,
        in_specs=placed,
        out_specs=(P(("groups", "ep"), None), P("groups")),
        check_vma=False,
    )
```
